32 devices in a mesh: img: 4 (over y, x), row: 8 (over z, core).
Axes of the slice: x: 2, y: 2, z: 4, core: 2. Of those that a mesh axis runs over, the one named last changes fastest.
Arguments:
- latent: bfloat16 [128, 128, 512], P(('img', 'row')), parts along dimension 0, may hold values from -8 to 8
- attn_gain: float32 [512], replicated, may hold values from 0.5 to 1.5
- attn_shift: float32 [512], replicated, may hold values from -3 to 3
- w_query: bfloat16 [512, 512], replicated, may hold values from -2 to 2
- w_key: bfloat16 [512, 512], replicated, may hold values from -2 to 2
- w_value: bfloat16 [512, 512], replicated, may hold values from -0.25 to 0.25
- w_out: bfloat16 [512, 512], replicated, may hold values from -0.25 to 0.25
- conv_gain: float32 [512], replicated, may hold values from 0.5 to 1.5
- conv_shift: float32 [512], replicated, may hold values from -3 to 3
- w_conv: bfloat16 [3, 3, 512, 512], replicated, may hold values from -0.09375 to 0.09375
- conv_bias: float32 [512], replicated, may hold values from -3 to 3
Outputs:
- encoded: bfloat16 [128, 128, 512], P(('img', 'row')), parts along dimension 0
The draws below stay inside these ranges and needn't reach their ends.
There are 4 independent parts, one for each index of `img`. The reference program is written for one: setup_inputs(seed, part) draws one part's arguments, and reference() takes and returns one part's arrays. A program takes and returns all parts, laid end to end along the dimension named above; an argument that names none is the same for every part. Nothing has to cross between parts.
All inputs are finite; a program needn't handle non-finite values.
Results may differ from the reference program's by a relative error of at most 0.011.
Values may be sent and summed in bfloat16 or wider, within the bound.
A program may use at most 128 MiB of HBM per device.

```python
import jax
import jax.numpy as jnp
from jax import lax

C = 512
GROUPS = 32
W = 128
H = 32


def shared_gauss(key):
    return jnp.clip(jax.random.normal(jax.random.fold_in(key, 7), (C, C), jnp.float32), -3.0, 3.0)


def draw_latent(key, part):
    noise = jax.random.normal(jax.random.fold_in(key, 3), (H, W, C), jnp.float32)
    rows = (jnp.arange(H, dtype=jnp.float32) + 0.5) / H
    phase = jax.random.uniform(jax.random.fold_in(key, 13), (GROUPS,), jnp.float32, -jnp.pi, jnp.pi)
    amplitude = jax.random.uniform(jax.random.fold_in(key, 17), (C,), jnp.float32, 0.8, 1.6)
    wave = jnp.sin(2.0 * jnp.pi * rows[:, None] + phase[None, :])
    offset = jnp.repeat(wave, C // GROUPS, axis=1) * amplitude[None, :]
    result = noise + offset[:, None, :]
    return jnp.clip(result, -8.0, 8.0).astype(jnp.bfloat16)


def draw_w_query(key, part):
    return (shared_gauss(key) * (4.0 / jnp.sqrt(jnp.float32(C)))).astype(jnp.bfloat16)


def draw_w_key(key, part):
    fresh = jnp.clip(jax.random.normal(jax.random.fold_in(key, 11), (C, C), jnp.float32), -3.0, 3.0)
    result = fresh / jnp.sqrt(jnp.float32(C))
    return result.astype(jnp.bfloat16)


def scatter_about(stream_key, extent, scale, most, kind=jnp.bfloat16):
    return jnp.clip(scale * jax.random.normal(stream_key, extent, jnp.float32), -most, most).astype(kind)


def setup_inputs(seed: int = 0, part: int = 0) -> dict:
    key_list = jax.random.split(jax.random.key(seed), 12)
    part_splits = jax.random.split(jax.random.fold_in(key_list[11], part), 12)
    return {
        "latent": draw_latent(jax.random.fold_in(jax.random.fold_in(key_list[11], part), 71), part),
        "attn_gain": jnp.clip(1.0 + 0.1 * jax.random.normal(key_list[1], (C,), jnp.float32), 0.5, 1.5),
        "attn_shift": scatter_about(key_list[2], (C,), 0.5, 3.0, jnp.float32),
        "w_query": draw_w_query(jax.random.fold_in(key_list[11], 71), part),
        "w_key": draw_w_key(jax.random.fold_in(key_list[11], 71), part),
        "w_value": scatter_about(key_list[5], (C, C), C ** -0.5, 0.25),
        "w_out": scatter_about(key_list[6], (C, C), C ** -0.5, 0.25),
        "conv_gain": jnp.clip(1.0 + 0.1 * jax.random.normal(key_list[7], (C,), jnp.float32), 0.5, 1.5),
        "conv_shift": scatter_about(key_list[8], (C,), 0.5, 3.0, jnp.float32),
        "w_conv": scatter_about(key_list[9], (3, 3, C, C), (9 * C) ** -0.5, 0.09375),
        "conv_bias": scatter_about(key_list[10], (C,), 0.5, 3.0, jnp.float32),
    }


epsilon = 1e-06

def group_norm(field, gain, shift):
    grouped = field.astype(jnp.float32).reshape(field.shape[0], GROUPS, C // GROUPS)
    centre = lax.optimization_barrier(jnp.mean(grouped, axis=(0, 2)))
    offset = grouped - centre[None, :, None]
    spread = lax.optimization_barrier(jnp.mean(offset * offset, axis=(0, 2)))
    normed = offset * lax.rsqrt(spread + epsilon)[None, :, None]
    return normed.reshape(field.shape) * gain + shift

def reference(latent, attn_gain, attn_shift, w_query, w_key, w_value, w_out, conv_gain, conv_shift, w_conv, conv_bias):
    positions = latent.reshape(H * W, C)
    normed = group_norm(positions, attn_gain, attn_shift).astype(jnp.bfloat16)
    queries = jnp.dot(normed, w_query, preferred_element_type=jnp.float32).astype(jnp.bfloat16)
    key_rows = jnp.dot(normed, w_key, preferred_element_type=jnp.float32).astype(jnp.bfloat16)
    values = jnp.dot(normed, w_value, preferred_element_type=jnp.float32).astype(jnp.bfloat16)
    scaling = 1.0 / jnp.sqrt(jnp.float32(C))
    scores = jnp.einsum('qc,kc->qk', queries.astype(jnp.float32), key_rows.astype(jnp.float32)) * scaling
    rowmax = lax.optimization_barrier(jnp.max(scores, axis=1))
    expo = jnp.exp(scores - rowmax[:, None])
    denominator = lax.optimization_barrier(jnp.sum(expo, axis=1))
    probs = expo.astype(jnp.bfloat16)
    attended = (jnp.dot(probs, values, preferred_element_type=jnp.float32) / denominator[:, None]).astype(jnp.bfloat16)
    hidden = (positions.astype(jnp.float32) + jnp.dot(attended, w_out, preferred_element_type=jnp.float32)).astype(jnp.bfloat16)
    activated = jax.nn.silu(group_norm(hidden, conv_gain, conv_shift)).astype(jnp.bfloat16).reshape(H, W, C)
    padded = jnp.pad(activated, ((1, 1), (1, 1), (0, 0)))
    convolved = jnp.zeros((H * W, C), jnp.float32)
    for row_tap in range(3):
        for col_tap in range(3):
            window = padded[row_tap:row_tap + H, col_tap:col_tap + W].reshape(H * W, C)
            convolved = convolved + jnp.dot(window, w_conv[row_tap, col_tap], preferred_element_type=jnp.float32)
    encoded = hidden.astype(jnp.float32) + (convolved + conv_bias)
    return encoded.astype(jnp.bfloat16).reshape(H, W, C)
```

```python
import functools
import math

import jax
import jax.numpy as jnp
from jax import lax
from jax.experimental import pallas as pl
from jax.experimental.pallas import tpu as pltpu
from jax.sharding import PartitionSpec as P

GROUPS = 32
EPS = 1e-06
CHUNK = 128
MESH = pl.DeviceIdType.MESH
LOG2E = math.log2(math.e)
NT = (((1,), (1,)), ((), ()))


def spread_groups(row, ones):
    high = row.astype(jnp.bfloat16).astype(jnp.float32)
    rest = row - high
    mid = rest.astype(jnp.bfloat16).astype(jnp.float32)
    low = rest - mid
    index = lax.broadcasted_iota(jnp.int32, (16, row.shape[1]), 0)
    parts = jnp.where(index == 0, high, jnp.where(index == 1, mid, jnp.where(index == 2, low, 0.0)))
    sums = jnp.dot(parts.astype(jnp.bfloat16), ones, preferred_element_type=jnp.float32)
    return jnp.sum(sums, axis=0, keepdims=True)


def kernel(
    n, wide,
    latent, w_query, w_key, w_value, w_out, w_conv,
    attn_gain, attn_shift, conv_gain, conv_shift, conv_bias,
    out,
    kv, wq, wk, wv, wo, wc, ones, moments, queries, bias, maxima, total, acc, hidden, halo, stacked,
    load_sem, weight_sem, send_sem, recv_sem, stat_send, stat_recv, halo_send, halo_recv,
):
    chunks, chunk, channels = kv.shape[1:]
    rows = chunks * chunk
    deep = n // 2
    lines = rows // wide
    size = channels // GROUPS
    img = lax.axis_index("img")
    r = lax.axis_index("row")
    z = r // 2
    c = r % 2
    partner = r + 1 - 2 * c

    loads = [
        pltpu.make_async_copy(latent.at[k], kv.at[r, k], load_sem.at[k]) for k in range(chunks)
    ]
    for load in loads:
        load.start()
    weights = [
        pltpu.make_async_copy(source, target, weight_sem.at[i])
        for i, (source, target) in enumerate([(w_query, wq), (w_key, wk), (w_value, wv), (w_out, wo)])
    ]
    weights += [
        pltpu.make_async_copy(
            w_conv.at[dy, dx],
            wc.at[dx, pl.ds(dy * channels, channels)],
            weight_sem.at[4 + dy * 3 + dx],
        )
        for dy in range(3)
        for dx in range(3)
    ]
    for weight in weights:
        weight.start()

    barrier = pltpu.get_barrier_semaphore()

    @pl.loop(1, n)
    def _(j):
        pl.semaphore_signal(
            barrier, inc=1, device_id=(img, lax.rem(r + j, n)), device_id_type=MESH
        )

    def piece(way, zb, k):
        b = zb * 2 + c
        target = (r + 2, r - 2, partner)[way]
        return pltpu.make_async_remote_copy(
            src_ref=kv.at[b, k],
            dst_ref=kv.at[b, k],
            send_sem=send_sem.at[way, zb, k],
            recv_sem=recv_sem.at[b, k],
            device_id=(img, target),
            device_id_type=MESH,
        )

    def arrival(b, k):
        return pltpu.make_async_remote_copy(
            src_ref=kv.at[b, k],
            dst_ref=kv.at[b, k],
            send_sem=send_sem.at[0, 0, 0],
            recv_sem=recv_sem.at[b, k],
            device_id=(img, partner),
            device_id_type=MESH,
        )

    def stat_copy(which, j):
        return pltpu.make_async_remote_copy(
            src_ref=moments.at[which, r],
            dst_ref=moments.at[which, r],
            send_sem=stat_send.at[which, j],
            recv_sem=stat_recv.at[which, r],
            device_id=(img, lax.rem(r + j, n)),
            device_id_type=MESH,
        )

    def stat_arrival(which, b):
        return pltpu.make_async_remote_copy(
            src_ref=moments.at[which, b],
            dst_ref=moments.at[which, b],
            send_sem=stat_send.at[which, 0],
            recv_sem=stat_recv.at[which, b],
            device_id=(img, partner),
            device_id_type=MESH,
        )

    def send_own(k):
        @pl.when(z < deep - 1)
        def _():
            piece(0, z, k).start()

        @pl.when(z > 0)
        def _():
            piece(1, z, k).start()

        piece(2, z, k).start()

    def share_moments(which, field):
        mean = jnp.sum(field, axis=0, keepdims=True) * (1.0 / rows)
        offset = field - mean
        square = jnp.sum(offset * offset, axis=0, keepdims=True)
        index = lax.broadcasted_iota(jnp.int32, (8, channels), 0)
        moments[which, r] = jnp.where(index == 0, mean, square)

        @pl.loop(1, n)
        def _(j):
            stat_copy(which, j).start()

    def gather_moments(which):
        @pl.loop(1, n)
        def _(j):
            stat_arrival(which, lax.rem(r + j, n)).wait_recv()

        @pl.loop(1, n)
        def _(j):
            stat_copy(which, j).wait_send()

        every = moments[which]
        means = every[:, 0, :]
        squares = every[:, 1, :]
        centre = spread_groups(jnp.sum(means, axis=0, keepdims=True), ones[...]) * (
            1.0 / (n * size)
        )
        away = means - centre
        whole = jnp.sum(squares + rows * (away * away), axis=0, keepdims=True)
        variance = spread_groups(whole, ones[...]) * (1.0 / (n * size * rows))
        return centre, lax.rsqrt(variance + EPS)

    left_group = lax.broadcasted_iota(jnp.int32, (channels, channels), 0) // size
    right_group = lax.broadcasted_iota(jnp.int32, (channels, channels), 1) // size
    ones[...] = jnp.where(left_group == right_group, 1.0, 0.0).astype(jnp.bfloat16)
    maxima[...] = jnp.full_like(maxima, -1e30)
    total[...] = jnp.zeros_like(total)
    acc[...] = jnp.zeros_like(acc)

    for load in loads:
        load.wait()
    pl.semaphore_wait(barrier, n - 1)
    send_own(0)
    share_moments(0, kv[r].reshape(rows, channels).astype(jnp.float32))
    for k in range(1, chunks):
        send_own(k)

    for weight in weights[:2]:
        weight.wait()
    centre, scale = gather_moments(0)
    gain = scale * attn_gain[...]
    positions = kv[r].reshape(rows, channels).astype(jnp.float32)
    normed = ((positions - centre) * gain + attn_shift[...]).astype(jnp.bfloat16)
    query = jnp.dot(normed, wq[...], preferred_element_type=jnp.float32).astype(jnp.bfloat16)
    folded = lax.dot_general(query, wk[...], NT, preferred_element_type=jnp.float32) * (
        LOG2E / math.sqrt(channels)
    )
    queries[...] = (folded * gain).astype(jnp.bfloat16)
    constant = jnp.sum(folded * (attn_shift[...] - centre * gain), axis=1, keepdims=True)
    bias[...] = jnp.broadcast_to(constant, bias.shape)

    def attend(b, k):
        block = kv[b, k]
        scores = lax.dot_general(queries[...], block, NT, preferred_element_type=jnp.float32)
        scores = scores + jnp.tile(bias[...], (1, chunk // 128))
        newest = jnp.maximum(maxima[...], jnp.max(scores, axis=1, keepdims=True))
        fade = jnp.exp2(maxima[...] - newest)
        maxima[...] = newest
        probs = jnp.exp2(scores - jnp.tile(newest, (1, chunk // 128))).astype(jnp.bfloat16)
        kept = probs.astype(jnp.float32)
        summed = total[...] * fade
        for j in range(chunk // 128):
            summed = summed + kept[:, j * 128 : (j + 1) * 128]
        total[...] = summed
        product = jnp.dot(probs, block, preferred_element_type=jnp.float32)
        acc[...] = acc[...] * jnp.tile(fade, (1, channels // 128)) + product

    @pl.loop(0, deep * chunks)
    def _(t):
        d = t // chunks
        k = t % chunks
        for way, zb in ((0, z - d), (1, z + d)):
            inside = jnp.logical_and(d > 0, jnp.logical_and(zb >= 0, zb < deep))

            @pl.when(inside)
            def _(way=way, zb=zb):
                arrival(zb * 2 + c, k).wait_recv()

                @pl.when((z < deep - 1) if way == 0 else (z > 0))
                def _():
                    piece(way, zb, k).start()

                piece(2, zb, k).start()

        @pl.loop(0, 4)
        def _(j):
            side = j % 2
            other = j // 2
            zb = z + d * (2 * side - 1)
            inside = jnp.logical_and(zb >= 0, zb < deep)

            @pl.when(jnp.logical_and(inside, jnp.logical_or(side == 0, d > 0)))
            def _():
                b = zb * 2 + c + other * (1 - 2 * c)

                @pl.when(other == 1)
                def _():
                    arrival(b, k).wait_recv()

                attend(b, k)

    for weight in weights[2:4]:
        weight.wait()
    denominator = jnp.sum(total[...], axis=1, keepdims=True)
    average = (acc[...] / denominator - centre) * gain + attn_shift[...]
    attended = jnp.dot(
        average.astype(jnp.bfloat16), wv[...], preferred_element_type=jnp.float32
    ).astype(jnp.bfloat16)
    field = (
        kv[r].reshape(rows, channels).astype(jnp.float32)
        + jnp.dot(attended, wo[...], preferred_element_type=jnp.float32)
    ).astype(jnp.bfloat16)
    hidden[...] = field
    share_moments(1, field.astype(jnp.float32))

    up = pltpu.make_async_remote_copy(
        src_ref=hidden.at[pl.ds(0, wide)],
        dst_ref=halo.at[1],
        send_sem=halo_send.at[1],
        recv_sem=halo_recv.at[1],
        device_id=(img, r - 1),
        device_id_type=MESH,
    )
    down = pltpu.make_async_remote_copy(
        src_ref=hidden.at[pl.ds(rows - wide, wide)],
        dst_ref=halo.at[0],
        send_sem=halo_send.at[0],
        recv_sem=halo_recv.at[0],
        device_id=(img, r + 1),
        device_id_type=MESH,
    )

    @pl.when(r > 0)
    def _():
        up.start()

    @pl.when(r < n - 1)
    def _():
        down.start()

    @pl.loop(0, deep * chunks)
    def _(t):
        zb = t // chunks
        k = t % chunks

        @pl.when(jnp.logical_and(z < deep - 1, zb <= z))
        def _():
            piece(0, zb, k).wait_send()

        @pl.when(jnp.logical_and(z > 0, zb >= z))
        def _():
            piece(1, zb, k).wait_send()

        piece(2, zb, k).wait_send()

    for weight in weights[4:]:
        weight.wait()
    centre, scale = gather_moments(1)
    gain = scale * conv_gain[...]

    def activate(values):
        v = (values.astype(jnp.float32) - centre) * gain + conv_shift[...]
        return (v / (1.0 + jnp.exp(-v))).astype(jnp.bfloat16)

    def place(line, values):
        for dy in range(3):
            y = line + 1 - dy
            if 0 <= y < lines:
                stacked[y * wide : (y + 1) * wide, dy * channels : (dy + 1) * channels] = values

    for line in range(lines):
        place(line, activate(hidden[line * wide : (line + 1) * wide]))

    @pl.when(r > 0)
    def _():
        up.wait_send()
        down.wait_recv()
        place(-1, activate(halo[0]))

    @pl.when(r == 0)
    def _():
        place(-1, jnp.zeros((wide, channels), jnp.bfloat16))

    @pl.when(r < n - 1)
    def _():
        down.wait_send()
        up.wait_recv()
        place(lines, activate(halo[1]))

    @pl.when(r == n - 1)
    def _():
        place(lines, jnp.zeros((wide, channels), jnp.bfloat16))

    half = 256
    column = lax.broadcasted_iota(jnp.int32, (rows, half), 0) % wide
    for start in range(0, channels, half):
        cut = slice(start, start + half)

        def taps(dx):
            return jnp.dot(stacked[...], wc[dx, :, cut], preferred_element_type=jnp.float32)

        convolved = taps(1)
        convolved = convolved + jnp.where(column > 0, pltpu.roll(taps(0), 1, 0), 0.0)
        convolved = convolved + jnp.where(
            column < wide - 1, pltpu.roll(taps(2), rows - 1, 0), 0.0
        )
        encoded = hidden[:, cut].astype(jnp.float32) + (convolved + conv_bias[:, cut])
        out[:, cut] = encoded.astype(jnp.bfloat16)


def local(n, latent, attn_gain, attn_shift, w_query, w_key, w_value, w_out,
          conv_gain, conv_shift, w_conv, conv_bias):
    height, wide, channels = latent.shape
    rows = height * wide
    chunks = rows // CHUNK
    anywhere = pl.BlockSpec(memory_space=pl.ANY)
    vmem = pl.BlockSpec(memory_space=pltpu.VMEM)
    bf16, f32 = jnp.bfloat16, jnp.float32
    square = pltpu.VMEM((channels, channels), bf16)
    dma = pltpu.SemaphoreType.DMA
    encoded = pl.pallas_call(
        functools.partial(kernel, n, wide),
        out_shape=jax.ShapeDtypeStruct((rows, channels), bf16),
        in_specs=[anywhere] * 6 + [vmem] * 5,
        out_specs=vmem,
        scratch_shapes=[
            pltpu.VMEM((n, chunks, CHUNK, channels), bf16),
            square, square, square, square,
            pltpu.VMEM((3, 3 * channels, channels), bf16),
            square,
            pltpu.VMEM((2, n, 8, channels), f32),
            pltpu.VMEM((rows, channels), bf16),
            pltpu.VMEM((rows, 128), f32),
            pltpu.VMEM((rows, 128), f32),
            pltpu.VMEM((rows, 128), f32),
            pltpu.VMEM((rows, channels), f32),
            pltpu.VMEM((rows, channels), bf16),
            pltpu.VMEM((2, wide, channels), bf16),
            pltpu.VMEM((rows, 3 * channels), bf16),
            dma((chunks,)),
            dma((13,)),
            dma((3, n // 2, chunks)),
            dma((n, chunks)),
            dma((2, n)),
            dma((2, n)),
            dma((2,)),
            dma((2,)),
        ],
        compiler_params=pltpu.CompilerParams(
            collective_id=0, has_side_effects=True, vmem_limit_bytes=56 * 1024 * 1024
        ),
    )(
        latent.reshape(chunks, CHUNK, channels), w_query, w_key, w_value, w_out, w_conv,
        *(v.reshape(1, channels) for v in (attn_gain, attn_shift, conv_gain, conv_shift, conv_bias)),
    )
    return encoded.reshape(height, wide, channels)


def solution(mesh):
    in_specs = (P(("img", "row"), None, None), P(), P(), P(), P(), P(), P(), P(), P(), P(), P())
    out_specs = P(("img", "row"), None, None)
    body = functools.partial(local, mesh.shape["row"])
    return jax.shard_map(body, mesh=mesh, in_specs=in_specs, out_specs=out_specs, check_vma=False)
```

```python
import functools
import math

import jax
import jax.numpy as jnp
from jax import lax
from jax.experimental import pallas as pl
from jax.experimental.pallas import tpu as pltpu
from jax.sharding import PartitionSpec as P

GROUPS = 32
EPS = 1e-06
CHUNK = 128
MESH = pl.DeviceIdType.MESH
LOG2E = math.log2(math.e)
NT = (((1,), (1,)), ((), ()))


def spread_groups(row, ones):
    high = row.astype(jnp.bfloat16).astype(jnp.float32)
    rest = row - high
    mid = rest.astype(jnp.bfloat16).astype(jnp.float32)
    low = rest - mid
    index = lax.broadcasted_iota(jnp.int32, (16, row.shape[1]), 0)
    parts = jnp.where(index == 0, high, jnp.where(index == 1, mid, jnp.where(index == 2, low, 0.0)))
    sums = jnp.dot(parts.astype(jnp.bfloat16), ones, preferred_element_type=jnp.float32)
    return jnp.sum(sums, axis=0, keepdims=True)


def kernel(
    n, wide,
    latent, w_query, w_key, w_value, w_out, w_conv,
    attn_gain, attn_shift, conv_gain, conv_shift, conv_bias,
    out,
    kv, wq, wk, wv, wo, wc, ones, moments, queries, bias, maxima, total, acc, hidden, halo, stacked,
    load_sem, weight_sem, send_sem, recv_sem, stat_send, stat_recv, halo_send, halo_recv,
    result, store_sem,
):
    chunks, chunk, channels = kv.shape[1:]
    rows = chunks * chunk
    deep = n // 2
    lines = rows // wide
    size = channels // GROUPS
    img = lax.axis_index("img")
    r = lax.axis_index("row")
    z = r // 2
    c = r % 2
    partner = r + 1 - 2 * c

    loads = [
        pltpu.make_async_copy(latent.at[k], kv.at[r, k], load_sem.at[k]) for k in range(chunks)
    ]
    for load in loads:
        load.start()
    weights = [
        pltpu.make_async_copy(source, target, weight_sem.at[i])
        for i, (source, target) in enumerate([(w_query, wq), (w_key, wk), (w_value, wv), (w_out, wo)])
    ]
    weights += [
        pltpu.make_async_copy(
            w_conv.at[dy, dx],
            wc.at[dx, pl.ds(dy * channels, channels)],
            weight_sem.at[4 + dy * 3 + dx],
        )
        for dy in range(3)
        for dx in range(3)
    ]
    for weight in weights:
        weight.start()

    barrier = pltpu.get_barrier_semaphore()

    @pl.loop(1, n)
    def _(j):
        pl.semaphore_signal(
            barrier, inc=1, device_id=(img, lax.rem(r + j, n)), device_id_type=MESH
        )

    def piece(way, zb, k):
        b = zb * 2 + c
        target = (r + 2, r - 2, partner)[way]
        return pltpu.make_async_remote_copy(
            src_ref=kv.at[b, k],
            dst_ref=kv.at[b, k],
            send_sem=send_sem.at[way, zb, k],
            recv_sem=recv_sem.at[b, k],
            device_id=(img, target),
            device_id_type=MESH,
        )

    def arrival(b, k):
        return pltpu.make_async_remote_copy(
            src_ref=kv.at[b, k],
            dst_ref=kv.at[b, k],
            send_sem=send_sem.at[0, 0, 0],
            recv_sem=recv_sem.at[b, k],
            device_id=(img, partner),
            device_id_type=MESH,
        )

    def stat_copy(which, j):
        return pltpu.make_async_remote_copy(
            src_ref=moments.at[which, r],
            dst_ref=moments.at[which, r],
            send_sem=stat_send.at[which, j],
            recv_sem=stat_recv.at[which, r],
            device_id=(img, lax.rem(r + j, n)),
            device_id_type=MESH,
        )

    def stat_arrival(which, b):
        return pltpu.make_async_remote_copy(
            src_ref=moments.at[which, b],
            dst_ref=moments.at[which, b],
            send_sem=stat_send.at[which, 0],
            recv_sem=stat_recv.at[which, b],
            device_id=(img, partner),
            device_id_type=MESH,
        )

    def send_own(k):
        @pl.when(z < deep - 1)
        def _():
            piece(0, z, k).start()

        @pl.when(z > 0)
        def _():
            piece(1, z, k).start()

        piece(2, z, k).start()

    def share_moments(which, field):
        mean = jnp.sum(field, axis=0, keepdims=True) * (1.0 / rows)
        offset = field - mean
        square = jnp.sum(offset * offset, axis=0, keepdims=True)
        moments[which, r, 0:1, :] = mean
        moments[which, r, 1:2, :] = square

        @pl.loop(1, n)
        def _(j):
            stat_copy(which, j).start()

    def gather_moments(which):
        @pl.loop(1, n)
        def _(j):
            stat_arrival(which, lax.rem(r + j, n)).wait_recv()

        @pl.loop(1, n)
        def _(j):
            stat_copy(which, j).wait_send()

        every = moments[which]
        means = every[:, 0, :]
        squares = every[:, 1, :]
        centre = spread_groups(jnp.sum(means, axis=0, keepdims=True), ones[...]) * (
            1.0 / (n * size)
        )
        away = means - centre
        whole = jnp.sum(squares + rows * (away * away), axis=0, keepdims=True)
        variance = spread_groups(whole, ones[...]) * (1.0 / (n * size * rows))
        return centre, lax.rsqrt(variance + EPS)

    for load in loads:
        load.wait()
    pl.semaphore_wait(barrier, n - 1)
    send_own(0)
    share_moments(0, kv[r].reshape(rows, channels).astype(jnp.float32))
    for k in range(1, chunks):
        send_own(k)

    left_group = lax.broadcasted_iota(jnp.int32, (channels, channels), 0) // size
    right_group = lax.broadcasted_iota(jnp.int32, (channels, channels), 1) // size
    ones[...] = jnp.where(left_group == right_group, 1.0, 0.0).astype(jnp.bfloat16)
    maxima[...] = jnp.full_like(maxima, -1e30)
    total[...] = jnp.zeros_like(total)
    acc[...] = jnp.zeros_like(acc)

    for weight in weights[:2]:
        weight.wait()
    centre, scale = gather_moments(0)
    gain = scale * attn_gain[...]
    positions = kv[r].reshape(rows, channels).astype(jnp.float32)
    normed = ((positions - centre) * gain + attn_shift[...]).astype(jnp.bfloat16)
    query = jnp.dot(normed, wq[...], preferred_element_type=jnp.float32).astype(jnp.bfloat16)
    folded = lax.dot_general(query, wk[...], NT, preferred_element_type=jnp.float32) * (
        LOG2E / math.sqrt(channels)
    )
    queries[...] = (folded * gain).astype(jnp.bfloat16)
    constant = jnp.sum(folded * (attn_shift[...] - centre * gain), axis=1, keepdims=True)
    bias[...] = jnp.broadcast_to(constant, bias.shape)

    def attend(b, k):
        block = kv[b, k]
        scores = lax.dot_general(queries[...], block, NT, preferred_element_type=jnp.float32)
        scores = scores + jnp.tile(bias[...], (1, chunk // 128))
        newest = jnp.maximum(maxima[...], jnp.max(scores, axis=1, keepdims=True))
        fade = jnp.exp2(maxima[...] - newest)
        maxima[...] = newest
        probs = jnp.exp2(scores - jnp.tile(newest, (1, chunk // 128))).astype(jnp.bfloat16)
        kept = probs.astype(jnp.float32)
        summed = total[...] * fade
        for j in range(chunk // 128):
            summed = summed + kept[:, j * 128 : (j + 1) * 128]
        total[...] = summed
        product = jnp.dot(probs, block, preferred_element_type=jnp.float32)
        acc[...] = acc[...] * jnp.tile(fade, (1, channels // 128)) + product

    def relay(t):
        d = t // chunks
        k = t % chunks
        for way, zb in ((0, z - d), (1, z + d)):
            inside = jnp.logical_and(d > 0, jnp.logical_and(zb >= 0, zb < deep))

            @pl.when(inside)
            def _(way=way, zb=zb):
                arrival(zb * 2 + c, k).wait_recv()

                @pl.when((z < deep - 1) if way == 0 else (z > 0))
                def _():
                    piece(way, zb, k).start()

                piece(2, zb, k).start()

    ahead = jnp.where(jnp.logical_and(z > 0, z < deep - 1), chunks, 0)

    @pl.loop(0, deep * chunks)
    def _(t):
        relay(t + ahead)
        d = t // chunks
        k = t % chunks

        @pl.loop(0, 4)
        def _(j):
            side = j % 2
            other = j // 2
            zb = z + d * (2 * side - 1)
            inside = jnp.logical_and(zb >= 0, zb < deep)

            @pl.when(jnp.logical_and(inside, jnp.logical_or(side == 0, d > 0)))
            def _():
                b = zb * 2 + c + other * (1 - 2 * c)

                @pl.when(other == 1)
                def _():
                    arrival(b, k).wait_recv()

                attend(b, k)

    for weight in weights[2:4]:
        weight.wait()
    denominator = jnp.sum(total[...], axis=1, keepdims=True)
    average = (acc[...] / denominator - centre) * gain + attn_shift[...]
    attended = jnp.dot(
        average.astype(jnp.bfloat16), wv[...], preferred_element_type=jnp.float32
    ).astype(jnp.bfloat16)
    field = (
        kv[r].reshape(rows, channels).astype(jnp.float32)
        + jnp.dot(attended, wo[...], preferred_element_type=jnp.float32)
    ).astype(jnp.bfloat16)
    hidden[...] = field
    share_moments(1, field.astype(jnp.float32))

    up = pltpu.make_async_remote_copy(
        src_ref=hidden.at[pl.ds(0, wide)],
        dst_ref=halo.at[1],
        send_sem=halo_send.at[1],
        recv_sem=halo_recv.at[1],
        device_id=(img, r - 1),
        device_id_type=MESH,
    )
    down = pltpu.make_async_remote_copy(
        src_ref=hidden.at[pl.ds(rows - wide, wide)],
        dst_ref=halo.at[0],
        send_sem=halo_send.at[0],
        recv_sem=halo_recv.at[0],
        device_id=(img, r + 1),
        device_id_type=MESH,
    )

    @pl.when(r > 0)
    def _():
        up.start()

    @pl.when(r < n - 1)
    def _():
        down.start()

    @pl.loop(0, deep * chunks)
    def _(t):
        zb = t // chunks
        k = t % chunks

        @pl.when(jnp.logical_and(z < deep - 1, zb <= z))
        def _():
            piece(0, zb, k).wait_send()

        @pl.when(jnp.logical_and(z > 0, zb >= z))
        def _():
            piece(1, zb, k).wait_send()

        piece(2, zb, k).wait_send()

    for weight in weights[4:]:
        weight.wait()
    centre, scale = gather_moments(1)
    gain = scale * conv_gain[...]

    def activate(values):
        v = (values.astype(jnp.float32) - centre) * gain + conv_shift[...]
        return (v / (1.0 + jnp.exp(-v))).astype(jnp.bfloat16)

    def place(line, values):
        for dy in range(3):
            y = line + 1 - dy
            if 0 <= y < lines:
                stacked[y * wide : (y + 1) * wide, dy * channels : (dy + 1) * channels] = values

    for line in range(lines):
        place(line, activate(hidden[line * wide : (line + 1) * wide]))

    @pl.when(r > 0)
    def _():
        up.wait_send()
        down.wait_recv()
        place(-1, activate(halo[0]))

    @pl.when(r == 0)
    def _():
        place(-1, jnp.zeros((wide, channels), jnp.bfloat16))

    @pl.when(r < n - 1)
    def _():
        down.wait_send()
        up.wait_recv()
        place(lines, activate(halo[1]))

    @pl.when(r == n - 1)
    def _():
        place(lines, jnp.zeros((wide, channels), jnp.bfloat16))

    half = 256
    stores = []
    column = lax.broadcasted_iota(jnp.int32, (rows, half), 0) % wide
    for start in range(0, channels, half):
        cut = slice(start, start + half)

        def taps(dx):
            return jnp.dot(stacked[...], wc[dx, :, cut], preferred_element_type=jnp.float32)

        convolved = taps(1)
        convolved = convolved + jnp.where(column > 0, pltpu.roll(taps(0), 1, 0), 0.0)
        convolved = convolved + jnp.where(
            column < wide - 1, pltpu.roll(taps(2), rows - 1, 0), 0.0
        )
        encoded = hidden[:, cut].astype(jnp.float32) + (convolved + conv_bias[:, cut])
        result[:, cut] = encoded.astype(jnp.bfloat16)
        store = pltpu.make_async_copy(
            result.at[:, cut], out.at[:, cut], store_sem.at[start // half]
        )
        store.start()
        stores.append(store)

    for store in stores:
        store.wait()


def local(n, latent, attn_gain, attn_shift, w_query, w_key, w_value, w_out,
          conv_gain, conv_shift, w_conv, conv_bias):
    height, wide, channels = latent.shape
    rows = height * wide
    chunks = rows // CHUNK
    anywhere = pl.BlockSpec(memory_space=pl.ANY)
    vmem = pl.BlockSpec(memory_space=pltpu.VMEM)
    bf16, f32 = jnp.bfloat16, jnp.float32
    square = pltpu.VMEM((channels, channels), bf16)
    dma = pltpu.SemaphoreType.DMA
    encoded = pl.pallas_call(
        functools.partial(kernel, n, wide),
        out_shape=jax.ShapeDtypeStruct((rows, channels), bf16),
        in_specs=[anywhere] * 6 + [vmem] * 5,
        out_specs=anywhere,
        scratch_shapes=[
            pltpu.VMEM((n, chunks, CHUNK, channels), bf16),
            square, square, square, square,
            pltpu.VMEM((3, 3 * channels, channels), bf16),
            square,
            pltpu.VMEM((2, n, 2, channels), f32),
            pltpu.VMEM((rows, channels), bf16),
            pltpu.VMEM((rows, 128), f32),
            pltpu.VMEM((rows, 128), f32),
            pltpu.VMEM((rows, 128), f32),
            pltpu.VMEM((rows, channels), f32),
            pltpu.VMEM((rows, channels), bf16),
            pltpu.VMEM((2, wide, channels), bf16),
            pltpu.VMEM((rows, 3 * channels), bf16),
            dma((chunks,)),
            dma((13,)),
            dma((3, n // 2, chunks)),
            dma((n, chunks)),
            dma((2, n)),
            dma((2, n)),
            dma((2,)),
            dma((2,)),
            pltpu.VMEM((rows, channels), bf16),
            dma((channels // 256,)),
        ],
        compiler_params=pltpu.CompilerParams(
            collective_id=0, has_side_effects=True, vmem_limit_bytes=56 * 1024 * 1024
        ),
    )(
        latent.reshape(chunks, CHUNK, channels), w_query, w_key, w_value, w_out, w_conv,
        *(v.reshape(1, channels) for v in (attn_gain, attn_shift, conv_gain, conv_shift, conv_bias)),
    )
    return encoded.reshape(height, wide, channels)


def solution(mesh):
    in_specs = (P(("img", "row"), None, None), P(), P(), P(), P(), P(), P(), P(), P(), P(), P())
    out_specs = P(("img", "row"), None, None)
    body = functools.partial(local, mesh.shape["row"])
    return jax.shard_map(body, mesh=mesh, in_specs=in_specs, out_specs=out_specs, check_vma=False)
```
